32 devices in a mesh: bond: 8 (over z, x), row: 4 (over y, core).
Axes of the slice: x: 2, y: 2, z: 4, core: 2. Of those that a mesh axis runs over, the one named last changes fastest.
Arguments:
- left_site: bfloat16 [16384, 1024], P(('bond', 'row')), may hold values from -6 to 6
- right_site: bfloat16 [8192, 2048], P(('bond', 'row')), may hold values from -0.1875 to 0.1875
- gate: float32 [4, 4], replicated, may hold values from -3 to 3
- omega: bfloat16 [2048, 1024], P(('bond', 'row')), may hold values from -0.125 to 0.125
Outputs:
- left_new: bfloat16 [16384, 1024], P(('bond', 'row'))
- right_new: bfloat16 [8192, 2048], P(('bond', 'row'))
- odd_pair: bfloat16 [16384, 2048], P(('bond', 'row'))
The draws below stay inside these ranges and needn't reach their ends.
All inputs are finite; a program needn't handle non-finite values.
Results may differ from the reference program's by a relative error of at most 0.03.
Values may be sent and summed in bfloat16 or wider, within the bound.
A program may use at most 128 MiB of HBM per device.

```python
import math
import jax
import jax.numpy as jnp
from jax import lax

C = 1024
K = 1024
BONDS = 8


def block_levels(rng, dims, shards, least, largest):
    factor_of = 1.0
    for position, parts in shards:
        heights = jax.random.uniform(jax.random.fold_in(jax.random.fold_in(rng, 6), position), (parts,), jnp.float32, least / len(shards), largest / len(shards))
        factor_of = factor_of * jnp.repeat(jnp.exp(heights), dims[position] // parts).reshape((-1,) + (1,) * (len(dims) - 1 - position))
    return factor_of


def noise(rng, shape, scale, bound, shards=(), kind=jnp.bfloat16):
    values = jax.random.normal(rng, shape, jnp.float32) * scale
    if len(shards) > 0:
        values = block_levels(rng, shape, shards, -0.22, 0.18) * values
    return jnp.clip(values, min=-bound, max=bound).astype(kind)


def setup_inputs(seed: int = 0) -> dict:
    key_list = jax.random.split(jax.random.key(seed), 5)
    return {
        "left_site": noise(key_list[0], (BONDS * 2 * C, C), 1.0, 6.0, ((0, 32),)),
        "right_site": noise(key_list[1], (BONDS * C, 2 * C), C ** -0.5, 0.1875, ((0, 32),)),
        "gate": noise(key_list[2], (4, 4), 0.5, 3.0, (), jnp.float32),
        "omega": noise(key_list[3], (2 * C, K), (2 * C) ** -0.5, 0.125, ((0, 32),)),
    }


def one_bond(pair_in, gate, omega):
    left_one, right_one = pair_in
    product = jnp.dot(left_one.astype(jnp.float32), right_one.astype(jnp.float32), preferred_element_type=jnp.float32)
    mixed = jnp.einsum('stuv,auvc->astc', gate.reshape(2, 2, 2, 2).astype(jnp.float32), product.reshape(C, 2, 2, 2 * C // 2))
    theta = mixed.reshape(2 * C, 2 * C).astype(jnp.bfloat16)
    sketch = jnp.dot(theta.astype(jnp.float32), omega.astype(jnp.float32), preferred_element_type=jnp.float32)
    gram = jnp.dot(sketch.T, sketch, precision=lax.Precision.HIGHEST) / (2.0 * C)
    diag_mean = jnp.trace(gram) / K
    lower = jnp.linalg.cholesky(gram + 0.01 * diag_mean * jnp.eye(K, dtype=gram.dtype))
    basis = lax.linalg.triangular_solve(lower, sketch, left_side=False, lower=True, transpose_a=True)
    left_out = basis.astype(jnp.bfloat16)
    right_out = (jnp.dot(left_out.T.astype(jnp.float32), theta.astype(jnp.float32), preferred_element_type=jnp.float32) * (1.0 / math.sqrt(2.0 * C))).astype(jnp.bfloat16)
    return (left_out, right_out)

def odd_bond(pair_in):
    right_one, left_next = pair_in
    rows_view = right_one.reshape(2 * K, C)
    cols_view = left_next.reshape(C, 2 * K)
    result = jnp.dot(rows_view.astype(jnp.float32), cols_view.astype(jnp.float32), preferred_element_type=jnp.float32) * (1.0 / math.sqrt(1.0 * C))
    return result.astype(jnp.bfloat16)

def reference(left_site, right_site, gate, omega):
    lefts = left_site.reshape(BONDS, 2 * C, C)
    rights = right_site.reshape(BONDS, C, 2 * C)
    left_out, right_out = lax.map(lambda pair_in: one_bond(pair_in, gate, omega), (lefts, rights))
    shifted = jnp.concatenate([left_out[1:], jnp.zeros((1, 2 * C, K), jnp.bfloat16)], axis=0)
    odd_pair = lax.map(odd_bond, (right_out, shifted))
    return (left_out.reshape(BONDS * 2 * C, K), right_out.reshape(BONDS * K, 2 * C), odd_pair.reshape(BONDS * 2 * K, 2 * K))
```

```python
import functools
import math

import jax
import jax.numpy as jnp
from jax import lax
from jax.experimental import pallas as pl
from jax.experimental.pallas import tpu as pltpu
from jax.sharding import PartitionSpec as P

LANES = 128
SUB = 8


def from_behind(block, axis, distance):
    devices = range(lax.axis_size(axis))
    route = [(i - distance, i) for i in devices if i - distance in devices]
    return lax.ppermute(block, axis, route)


def split(x):
    high = x.astype(jnp.bfloat16)
    return high, (x - high.astype(jnp.float32)).astype(jnp.bfloat16)


def inverse_factor(block):
    groups = LANES // SUB
    lane = lax.broadcasted_iota(jnp.int32, (SUB, LANES), 1)
    sub = lax.broadcasted_iota(jnp.int32, (SUB, LANES), 0)
    left = [block[g * SUB:(g + 1) * SUB, :] for g in range(groups)]
    right = [jnp.where(lane == sub + g * SUB, 1.0, 0.0) for g in range(groups)]
    rows = []

    def over_lanes(x, column):
        return jnp.broadcast_to(x[:, column:column + 1], (SUB, LANES))

    def over_rows(x, row):
        return jnp.broadcast_to(x[row:row + 1, :], (SUB, LANES))

    for g in range(groups):
        a, e = left[g], right[g]
        cols = [over_lanes(a, g * SUB + c) for c in range(SUB)]
        finished = jnp.zeros_like(e)
        for k in range(SUB):
            here = sub == k
            pivot = over_rows(cols[k], k)
            inverse = 1.0 / pivot
            factor = cols[k] * inverse
            row_a, row_e = over_rows(a, k), over_rows(e, k)
            finished = jnp.where(here, row_e * lax.rsqrt(pivot), finished)
            a = jnp.where(here, row_a * inverse, a - factor * row_a)
            e = jnp.where(here, row_e * inverse, e - factor * row_e)
            for c in range(k + 1, SUB):
                row_c = over_rows(cols[c], k)
                cols[c] = jnp.where(here, row_c * inverse, cols[c] - factor * row_c)
        rows.append(finished)
        if g + 1 == groups:
            break
        wide_a = [over_rows(a, k) for k in range(SUB)]
        wide_e = [over_rows(e, k) for k in range(SUB)]
        for i in range(g + 1, groups):
            coeff = [over_lanes(left[i], g * SUB + c) for c in range(SUB)]
            for c in range(SUB):
                left[i] = left[i] - coeff[c] * wide_a[c]
                right[i] = right[i] - coeff[c] * wide_e[c]
    return jnp.concatenate(rows, axis=0)


def solve_kernel(scale, gram_ref, sketch_ref, flat_ref, tall_ref, work, wide):
    size = gram_ref.shape[0]
    blocks = size // LANES
    width = size + sketch_ref.shape[1]
    eye = (
        lax.broadcasted_iota(jnp.int32, (LANES, LANES), 0)
        == lax.broadcasted_iota(jnp.int32, (LANES, LANES), 1)
    )

    total = jnp.zeros((LANES, LANES), jnp.float32)
    for d in range(blocks):
        at = slice(d * LANES, (d + 1) * LANES)
        total = total + jnp.where(eye, gram_ref[at, at], 0.0)
    ridge = jnp.sum(total, keepdims=True) * (scale * 0.01 / size)
    for d in range(blocks):
        at = slice(d * LANES, (d + 1) * LANES)
        work[at, :size] = gram_ref[at, :] * scale
        work[at, size:] = sketch_ref[at, :]
        work[at, at] = work[at, at] + jnp.where(eye, ridge, 0.0)

    def eliminate(d, carry):
        start = pl.multiple_of(d * LANES, LANES)
        here = pl.ds(start, LANES)
        inverse = inverse_factor(work[here, here])
        high, low = split(inverse)
        factor = jnp.concatenate([high, high, low], axis=1)
        high, low = split(work[here, :])
        solved = jnp.dot(
            factor,
            jnp.concatenate([high, low, high], axis=0),
            preferred_element_type=jnp.float32,
        )
        work[here, :] = solved
        high, low = split(solved)
        wide[0:LANES, :] = high
        wide[LANES:2 * LANES, :] = low
        wide[2 * LANES:, :] = high
        basis = solved[:, size:]
        flat_ref[here, :] = basis.astype(jnp.bfloat16)
        tall_ref[:, here] = basis.T.astype(jnp.bfloat16)

        def update(i, carry):
            there = pl.ds(pl.multiple_of(i * LANES, LANES), LANES)
            high, low = split(work[here, there].T)
            lower = jnp.concatenate([high, high, low], axis=1)
            work[there, :] = work[there, :] - jnp.dot(
                lower, wide[...], preferred_element_type=jnp.float32
            )
            return carry

        return lax.fori_loop(d + 1, blocks, update, carry)

    lax.fori_loop(0, blocks, eliminate, 0)


def solve(gram, sketch_t, scale):
    size, rows = sketch_t.shape
    return pl.pallas_call(
        functools.partial(solve_kernel, scale),
        out_shape=(
            jax.ShapeDtypeStruct((size, rows), jnp.bfloat16),
            jax.ShapeDtypeStruct((rows, size), jnp.bfloat16),
        ),
        in_specs=[pl.BlockSpec(memory_space=pltpu.VMEM)] * 2,
        out_specs=(pl.BlockSpec(memory_space=pltpu.VMEM),) * 2,
        scratch_shapes=[
            pltpu.VMEM((size, size + rows), jnp.float32),
            pltpu.VMEM((3 * LANES, size + rows), jnp.bfloat16),
        ],
        compiler_params=pltpu.CompilerParams(vmem_limit_bytes=48 * 1024 * 1024),
        cost_estimate=pl.CostEstimate(
            flops=4 * size * size * (size + rows), bytes_accessed=4 * size * (size + 2 * rows), transcendentals=size
        ),
        name="solve",
    )(gram, sketch_t)


def shards(left_site, right_site, gate, omega):
    row_count = left_site.shape[0]
    bond_width = left_site.shape[1]
    kept_rank = omega.shape[1]
    product = jnp.dot(
        left_site,
        lax.all_gather(right_site, "row", axis=0, tiled=True),
        preferred_element_type=jnp.float32,
    )
    mixed = jnp.einsum(
        "stuv,auvc->astc",
        gate.reshape(2, 2, 2, 2),
        product.reshape(row_count // 2, 2, 2, bond_width),
    )
    theta = mixed.reshape(row_count, 2 * bond_width).astype(jnp.bfloat16)
    sketch_t = lax.dot_general(
        lax.all_gather(omega, ("bond", "row"), axis=0, tiled=True),
        theta,
        (((0,), (1,)), ((), ())),
        preferred_element_type=jnp.float32,
    )
    high, low = split(sketch_t)
    over = (((1,), (1,)), ((), ()))
    local_gram = lax.dot_general(
        jnp.concatenate([high, high, low], axis=1),
        jnp.concatenate([high, low, high], axis=1),
        over,
        preferred_element_type=jnp.float32,
    )
    gram = lax.psum(local_gram, "row")
    left_t, left_new = solve(gram, sketch_t, 1.0 / (2.0 * bond_width))
    right_scale = 1.0 / math.sqrt(2.0 * bond_width)
    own_rows = kept_rank // lax.axis_size("row")
    following = from_behind(left_new.reshape(row_count // 2, 2 * kept_rank), "bond", -1)
    right_new = lax.psum_scatter(
        (jnp.dot(left_t, theta, preferred_element_type=jnp.float32) * right_scale).astype(jnp.bfloat16),
        "row",
        scatter_dimension=0,
        tiled=True,
    )
    right_view = right_new.reshape(2 * own_rows, bond_width)
    pair_sum = jnp.dot(
        right_view,
        lax.all_gather(following, "row", axis=0, tiled=True),
        preferred_element_type=jnp.float32,
    )
    odd_pair = (pair_sum * (1.0 / math.sqrt(1.0 * bond_width))).astype(jnp.bfloat16)
    return (left_new, right_new, odd_pair)


def solution(mesh):
    placed = (P(("bond", "row"), None), P(("bond", "row"), None), P(), P(("bond", "row"), None))
    return jax.shard_map(
        shards,
        mesh=mesh,
        in_specs=placed,
        out_specs=(P(("bond", "row"), None), P(("bond", "row"), None), P(("bond", "row"), None)),
        check_vma=False,
    )
```

```python
import functools
import math

import jax
import jax.numpy as jnp
from jax import lax
from jax.experimental import pallas as pl
from jax.experimental.pallas import tpu as pltpu
from jax.sharding import PartitionSpec as P

LANES = 128
SUB = 8


MESH = pl.DeviceIdType.MESH
CHUNKS = 8


def partner(me, distance):
    span = 2 * distance
    return lax.div(me, span) * span + lax.rem(lax.rem(me, span) + distance, span)


def distances(n):
    found = []
    while n > 1:
        n //= 2
        found.append(n)
    return found


def gather_kernel(axis, n, last, block_ref, out_ref, send_sem, recv_sem):
    shifted = last is not None
    me = lax.axis_index(axis)
    rows = block_ref.shape[0]
    piece = rows // CHUNKS
    steps = distances(n)

    barrier = pltpu.get_barrier_semaphore()
    for s in steps:
        pl.semaphore_signal(barrier, inc=1, device_id={axis: partner(me, s)}, device_id_type=MESH)
    if shifted:
        bond = lax.axis_index("bond")
        for way in (1, last):
            to = lax.rem(bond + way, last + 1)
            pl.semaphore_signal(barrier, inc=1, device_id={"bond": to}, device_id_type=MESH)
    pl.semaphore_wait(barrier, len(steps) + (2 if shifted else 0))

    def owner(mask):
        at = me
        for s in steps:
            if mask & s:
                at = partner(at, s)
        return at

    def slot(mask, k):
        start = pl.multiple_of(owner(mask) * rows + k * piece, piece)
        return out_ref.at[pl.ds(start, piece), :]

    def own(k):
        return block_ref.at[k * piece:(k + 1) * piece, :]

    def copy(mask, s, k):
        source = slot(mask, k) if mask or shifted else own(k)
        return pltpu.make_async_remote_copy(
            src_ref=source,
            dst_ref=slot(mask, k),
            send_sem=send_sem.at[mask + s, k],
            recv_sem=recv_sem.at[mask + s, k],
            device_id={axis: partner(me, s)},
            device_id_type=MESH,
        )

    def behind(k):
        return pltpu.make_async_remote_copy(
            src_ref=own(k),
            dst_ref=slot(0, k),
            send_sem=send_sem.at[0, k],
            recv_sem=recv_sem.at[0, k],
            device_id={"bond": bond - 1},
            device_id_type=MESH,
        )

    def lower_steps(mask):
        return [s for s in steps if mask == 0 or s < (mask & -mask)]

    order = [m for s in steps for m in range(s, n, 2 * s)]

    def spread():
        for s in steps:
            for k in range(CHUNKS):
                if shifted and s == steps[0]:
                    behind(k).wait_recv()
                copy(0, s, k).start()
        for mask in order:
            for k in range(CHUNKS):
                copy(mask - (mask & -mask), mask & -mask, k).wait_recv()
                for s in lower_steps(mask):
                    copy(mask, s, k).start()
        for mask in [0] + order:
            for s in lower_steps(mask):
                for k in range(CHUNKS):
                    copy(mask, s, k).wait_send()

    if not shifted:
        start = pl.multiple_of(me * rows, rows)
        spread()
        out_ref[pl.ds(start, rows), :] = block_ref[...]
        return

    @pl.when(bond > 0)
    def _():
        for k in range(CHUNKS):
            behind(k).start()

    @pl.when(bond < last)
    def _():
        spread()

    @pl.when(bond == last)
    def _():
        out_ref[...] = jnp.zeros_like(out_ref)

    @pl.when(bond > 0)
    def _():
        for k in range(CHUNKS):
            behind(k).wait_send()


def gather(block, axis, n, last, number):
    rows, columns = block.shape
    return pl.pallas_call(
        functools.partial(gather_kernel, axis, n, last),
        out_shape=jax.ShapeDtypeStruct((n * rows, columns), block.dtype),
        in_specs=[pl.BlockSpec(memory_space=pltpu.VMEM)],
        out_specs=pl.BlockSpec(memory_space=pltpu.VMEM),
        scratch_shapes=[pltpu.SemaphoreType.DMA((n, CHUNKS)), pltpu.SemaphoreType.DMA((n, CHUNKS))],
        compiler_params=pltpu.CompilerParams(
            collective_id=number, has_side_effects=True, vmem_limit_bytes=16 * 1024 * 1024
        ),
        cost_estimate=pl.CostEstimate(flops=0, bytes_accessed=100 * 1024 * 1024, transcendentals=0),
        name="gather",
    )(block)


def split(x):
    high = x.astype(jnp.bfloat16)
    return high, (x - high.astype(jnp.float32)).astype(jnp.bfloat16)


def inverse_factor(block):
    groups = LANES // SUB
    lane = lax.broadcasted_iota(jnp.int32, (SUB, LANES), 1)
    sub = lax.broadcasted_iota(jnp.int32, (SUB, LANES), 0)
    left = [block[g * SUB:(g + 1) * SUB, :] for g in range(groups)]
    right = [jnp.where(lane == sub + g * SUB, 1.0, 0.0) for g in range(groups)]
    rows = []

    def over_lanes(x, column):
        return jnp.broadcast_to(x[:, column:column + 1], (SUB, LANES))

    def over_rows(x, row):
        return jnp.broadcast_to(x[row:row + 1, :], (SUB, LANES))

    for g in range(groups):
        a, e = left[g], right[g]
        cols = [over_lanes(a, g * SUB + c) for c in range(SUB)]
        finished = jnp.zeros_like(e)
        for k in range(SUB):
            here = sub == k
            pivot = over_rows(cols[k], k)
            inverse = 1.0 / pivot
            factor = cols[k] * inverse
            row_a, row_e = over_rows(a, k), over_rows(e, k)
            finished = jnp.where(here, row_e * lax.rsqrt(pivot), finished)
            a = jnp.where(here, row_a * inverse, a - factor * row_a)
            e = jnp.where(here, row_e * inverse, e - factor * row_e)
            for c in range(k + 1, SUB):
                row_c = over_rows(cols[c], k)
                cols[c] = jnp.where(here, row_c * inverse, cols[c] - factor * row_c)
        rows.append(finished)
        if g + 1 == groups:
            break
        wide_a = [over_rows(a, k) for k in range(SUB)]
        wide_e = [over_rows(e, k) for k in range(SUB)]
        for i in range(g + 1, groups):
            coeff = [over_lanes(left[i], g * SUB + c) for c in range(SUB)]
            for c in range(SUB):
                left[i] = left[i] - coeff[c] * wide_a[c]
                right[i] = right[i] - coeff[c] * wide_e[c]
    return jnp.concatenate(rows, axis=0)


def add_up(n, gram_ref, work, near, far, sums, others, send_sem, recv_sem):
    size = gram_ref.shape[0]
    blocks, half = size // LANES, LANES // 2
    me = lax.axis_index("row")
    steps = distances(n)[::-1]
    mine = lax.rem(me, 2)

    barrier = pltpu.get_barrier_semaphore()
    for s in steps:
        pl.semaphore_signal(barrier, inc=1, device_id={"row": partner(me, s)}, device_id_type=MESH)
    pl.semaphore_wait(barrier, len(steps))

    def rows(i, side):
        return pl.ds(pl.multiple_of(i * LANES + side * half, half), half)

    def copy(source, target, stage, s, i):
        return pltpu.make_async_remote_copy(
            src_ref=source,
            dst_ref=target,
            send_sem=send_sem.at[stage, i],
            recv_sem=recv_sem.at[stage, i],
            device_id={"row": partner(me, s)},
            device_id_type=MESH,
        )

    def packed(ref, i):
        return ref.at[i * half:(i + 1) * half, i * LANES:]

    def first(i):
        return copy(gram_ref.at[rows(i, 1 - mine), i * LANES:], packed(near, i), 0, 1, i)

    def across(j, i):
        return copy(packed(sums, i), packed(far.at[j], i), j + 1, steps[j + 1], i)

    def back(i):
        return copy(packed(sums, i), packed(others, i), len(steps), 1, i)

    for i in range(blocks):
        first(i).start()
    for i in range(blocks):
        first(i).wait()
        packed(sums, i)[...] = gram_ref[rows(i, mine), i * LANES:] + packed(near, i)[...]
        if len(steps) > 1:
            across(0, i).start()
        else:
            back(i).start()
    for j in range(len(steps) - 1):
        for i in range(blocks):
            across(j, i).wait()
            packed(sums, i)[...] = packed(sums, i)[...] + packed(far.at[j], i)[...]
            if j + 2 < len(steps):
                across(j + 1, i).start()
            else:
                back(i).start()
    for i in range(blocks):
        back(i).wait()
        work[rows(i, mine), i * LANES:size] = packed(sums, i)[...]
        work[rows(i, 1 - mine), i * LANES:size] = packed(others, i)[...]


def solve_kernel(scale, n, gram_ref, sketch_ref, flat_ref, tall_ref, work, wide, *exchange):
    size = gram_ref.shape[0]
    blocks = size // LANES
    width = size + sketch_ref.shape[1]
    eye = (
        lax.broadcasted_iota(jnp.int32, (LANES, LANES), 0)
        == lax.broadcasted_iota(jnp.int32, (LANES, LANES), 1)
    )

    for d in range(1, blocks):
        work[d * LANES:(d + 1) * LANES, :d * LANES] = jnp.zeros((LANES, d * LANES), jnp.float32)
    work[:, size:] = sketch_ref[...]
    add_up(n, gram_ref, work, *exchange)
    total = jnp.zeros((LANES, LANES), jnp.float32)
    for d in range(blocks):
        at = slice(d * LANES, (d + 1) * LANES)
        total = total + jnp.where(eye, work[at, at], 0.0)
    ridge = jnp.sum(total, keepdims=True) * (scale * 0.01 / size)
    for d in range(blocks):
        at = slice(d * LANES, (d + 1) * LANES)
        work[at, d * LANES:size] = work[at, d * LANES:size] * scale
        work[at, at] = work[at, at] + jnp.where(eye, ridge, 0.0)

    def eliminate(d, carry):
        start = pl.multiple_of(d * LANES, LANES)
        here = pl.ds(start, LANES)
        inverse = inverse_factor(work[here, here])
        high, low = split(inverse)
        factor = jnp.concatenate([high, high, low], axis=1)
        high, low = split(work[here, :])
        solved = jnp.dot(
            factor,
            jnp.concatenate([high, low, high], axis=0),
            preferred_element_type=jnp.float32,
        )
        work[here, :] = solved
        high, low = split(solved)
        wide[0:LANES, :] = high
        wide[LANES:2 * LANES, :] = low
        wide[2 * LANES:, :] = high
        basis = solved[:, size:]
        flat_ref[here, :] = basis.astype(jnp.bfloat16)
        tall_ref[:, here] = basis.T.astype(jnp.bfloat16)

        def update(i, carry):
            there = pl.ds(pl.multiple_of(i * LANES, LANES), LANES)
            high, low = split(work[here, there].T)
            lower = jnp.concatenate([high, high, low], axis=1)
            work[there, :] = work[there, :] - jnp.dot(
                lower, wide[...], preferred_element_type=jnp.float32
            )
            return carry

        return lax.fori_loop(d + 1, blocks, update, carry)

    lax.fori_loop(0, blocks, eliminate, 0)


def solve(gram, sketch_t, scale, n, number):
    size, rows = sketch_t.shape
    stages = len(distances(n)) + 1
    packed = (size // 2, size)
    return pl.pallas_call(
        functools.partial(solve_kernel, scale, n),
        out_shape=(
            jax.ShapeDtypeStruct((size, rows), jnp.bfloat16),
            jax.ShapeDtypeStruct((rows, size), jnp.bfloat16),
        ),
        in_specs=[pl.BlockSpec(memory_space=pltpu.VMEM)] * 2,
        out_specs=(pl.BlockSpec(memory_space=pltpu.VMEM),) * 2,
        scratch_shapes=[
            pltpu.VMEM((size, size + rows), jnp.float32),
            pltpu.VMEM((3 * LANES, size + rows), jnp.bfloat16),
            pltpu.VMEM(packed, jnp.float32),
            pltpu.VMEM((max(stages - 2, 1),) + packed, jnp.float32),
            pltpu.VMEM(packed, jnp.float32),
            pltpu.VMEM(packed, jnp.float32),
            pltpu.SemaphoreType.DMA((stages, size // LANES)),
            pltpu.SemaphoreType.DMA((stages, size // LANES)),
        ],
        compiler_params=pltpu.CompilerParams(
            collective_id=number, has_side_effects=True, vmem_limit_bytes=48 * 1024 * 1024
        ),
        cost_estimate=pl.CostEstimate(
            flops=4 * size * size * (size + rows), bytes_accessed=4 * size * (size + 2 * rows), transcendentals=size
        ),
        name="solve",
    )(gram, sketch_t)


def shards(left_site, right_site, gate, omega):
    row_count = left_site.shape[0]
    bond_width = left_site.shape[1]
    kept_rank = omega.shape[1]
    group = lax.axis_size("row")
    product = jnp.dot(
        left_site,
        gather(right_site, "row", group, None, 0),
        preferred_element_type=jnp.float32,
    )
    mixed = jnp.einsum(
        "stuv,auvc->astc",
        gate.reshape(2, 2, 2, 2),
        product.reshape(row_count // 2, 2, 2, bond_width),
    )
    theta = mixed.reshape(row_count, 2 * bond_width).astype(jnp.bfloat16)
    sketch_t = lax.dot_general(
        lax.all_gather(omega, ("bond", "row"), axis=0, tiled=True),
        theta,
        (((0,), (1,)), ((), ())),
        preferred_element_type=jnp.float32,
    )
    high, low = split(sketch_t)
    over = (((1,), (1,)), ((), ()))
    local_gram = lax.dot_general(
        jnp.concatenate([high, high, low], axis=1),
        jnp.concatenate([high, low, high], axis=1),
        over,
        preferred_element_type=jnp.float32,
    )
    left_t, left_new = solve(local_gram, sketch_t, 1.0 / (2.0 * bond_width), group, 1)
    right_scale = 1.0 / math.sqrt(2.0 * bond_width)
    own_rows = kept_rank // group
    partial = (jnp.dot(left_t, theta, preferred_element_type=jnp.float32) * right_scale).astype(jnp.bfloat16)
    partial, ahead = lax.optimization_barrier((partial, left_new))
    right_new = lax.psum_scatter(partial, "row", scatter_dimension=0, tiled=True)
    following = gather(
        ahead.reshape(row_count // 2, 2 * kept_rank), "row", group, lax.axis_size("bond") - 1, 2
    )
    right_view = right_new.reshape(2 * own_rows, bond_width)
    pair_sum = jnp.dot(
        right_view,
        following,
        preferred_element_type=jnp.float32,
    )
    odd_pair = (pair_sum * (1.0 / math.sqrt(1.0 * bond_width))).astype(jnp.bfloat16)
    return (left_new, right_new, odd_pair)


def solution(mesh):
    placed = (P(("bond", "row"), None), P(("bond", "row"), None), P(), P(("bond", "row"), None))
    return jax.shard_map(
        shards,
        mesh=mesh,
        in_specs=placed,
        out_specs=(P(("bond", "row"), None), P(("bond", "row"), None), P(("bond", "row"), None)),
        check_vma=False,
    )
```
